32 devices in a mesh: dp: 8 (over z, y), tensor: 4 (over x, core).
Axes of the slice: x: 2, y: 2, z: 4, core: 2. Of those that a mesh axis runs over, the one named last changes fastest.
Arguments:
- attn_out: bfloat16 [2048, 4096], P('dp', 'tensor'), may hold values from -6 to 6
- w_blocks: bfloat16 [4096, 8192], P('tensor', 'dp'), may hold values from -0.09375 to 0.09375
- w_scales: float32 [32, 8192], P('tensor', 'dp'), may hold values from 0.5 to 2
- residual: bfloat16 [2048, 8192], P('dp')
- gain: float32 [8192], P('tensor'), may hold values from 0.5 to 1.5
Outputs:
- hidden: bfloat16 [2048, 8192], P('dp', 'tensor')
- normed: bfloat16 [2048, 8192], P('dp', 'tensor')
The draws below stay inside these ranges and needn't reach their ends.
All inputs are finite; a program needn't handle non-finite values.
Results may differ from the reference program's by a relative error of at most 0.014.
Values may be sent and summed in bfloat16 or wider, within the bound.
A program may use at most 128 MiB of HBM per device.

```python
import math
import jax
import jax.numpy as jnp
from jax import lax

D = 8192
BLOCK = 128
HD = 4096
TOKENS = 2048


def draw_residual(key, part):
    first = jax.random.fold_in(jax.random.fold_in(key, 17), 0)
    base = jnp.clip(jax.random.normal(first, (TOKENS, D), jnp.float32), -6.0, 6.0)
    ramp = 0.6 * jnp.exp(math.log(3.0) * jnp.arange(D, dtype=jnp.float32) / D)
    return (base * ramp[None, :]).astype(jnp.bfloat16)


def shard_levels(rng, extent, shards, smallest, high):
    level, own = 1.0, jax.random.fold_in(rng, 6)
    for dim, parts in shards:
        heights = jnp.exp(jax.random.uniform(jax.random.fold_in(own, dim), (parts,), jnp.float32, smallest / len(shards), high / len(shards)))
        level = level * jnp.repeat(heights, extent[dim] // parts).reshape([-1 if axis == dim else 1 for axis in range(len(extent))])
    return level


def bell_draw(own_key, shape, scale, most, cuts=(), held_as=jnp.bfloat16):
    values = jax.random.normal(own_key, shape, jnp.float32) * scale
    if len(cuts) > 0:
        values = shard_levels(own_key, shape, cuts, -0.22, 0.18) * values
    return jnp.clip(values, min=-most, max=most).astype(held_as)


def setup_inputs(seed: int = 0) -> dict:
    key_list = jax.random.split(jax.random.key(seed), 6)
    attn_out = bell_draw(key_list[0], (TOKENS, HD), 1.0, 6.0, ((0, 8), (1, 4)))
    w_blocks = bell_draw(key_list[1], (HD, D), HD ** -0.5, 0.09375, ((0, 4), (1, 8)))
    w_scales = jnp.clip(jnp.exp(math.log(2.0) - 1.3862944 * jax.random.uniform(key_list[2], (HD // BLOCK, D), jnp.float32) ** shard_levels(key_list[2], (HD // BLOCK, D), ((0, 4), (1, 8)), -0.2, 0.2)), 0.5, 2.0)
    residual = draw_residual(jax.random.fold_in(key_list[5], 71), 0)
    gain = jnp.clip(1.0 + 0.1 * jax.random.normal(key_list[4], (D,), jnp.float32), 0.5, 1.5)
    return {"attn_out": attn_out, "w_blocks": w_blocks, "w_scales": w_scales, "residual": residual, "gain": gain}


def dequantize(blocks, scales):
    spread = jnp.repeat(scales, BLOCK, axis=0)
    return (blocks.astype(jnp.float32) * spread).astype(jnp.bfloat16)

def reference(attn_out, w_blocks, w_scales, residual, gain):
    weights = dequantize(w_blocks, w_scales)
    attn_sum = jnp.dot(attn_out, weights, preferred_element_type=jnp.float32)
    hidden = (residual.astype(jnp.float32) + attn_sum).astype(jnp.bfloat16)
    wide = hidden.astype(jnp.float32)
    mean_square = lax.optimization_barrier(jnp.sum(wide * wide, axis=1, keepdims=True)) / D
    normed = (wide * gain[None, :] * jax.lax.rsqrt(mean_square + 1e-05)).astype(jnp.bfloat16)
    return (hidden, normed)
```

```python
import functools

import jax
import jax.numpy as jnp
from jax import lax
from jax.experimental import pallas as pl
from jax.experimental.pallas import tpu as pltpu
from jax.sharding import PartitionSpec as P

MESH = pl.DeviceIdType.MESH
WIDTH = 256
LANES = 128
PARTS = 2


def plan(dp, groups, cols):
    inner = dp // groups
    width = min(WIDTH, cols)
    pieces = [(0, c, width) for c in range(0, cols, width)]
    own = len(pieces)
    for r in range(1, inner):
        for c in range(0, cols, width):
            if r == inner - 1 and c == cols - width and width > LANES:
                pieces += [(r, k, LANES) for k in range(c, cols, LANES)]
            else:
                pieces.append((r, c, width))
    total = (inner - 1) * cols
    level, done = [0] * own, 0
    for _, _, w in pieces[own:]:
        done += w
        level.append(1 + (done * groups - 1) // total)
    last = [s for s, at in enumerate(level) if at >= groups]
    for k, s in enumerate(last):
        level[s] = groups + (2 * k) // len(last)
    waves = [[] for _ in range(groups + 2)]
    for j in range(groups):
        for s, at in enumerate(level):
            waves[max(j, at)].append((j, s))
    return inner, width, pieces, own, level, waves


def kernel(
    dp, groups,
    a_hbm, w_hbm, sc_hbm, res_hbm,
    hidden, scl,
    a_buf, w_buf, sc_buf, wd, res,
    keep1, snd1, rcv1, snd2, keep2, rcv2, snd3, zin, hs, acc, scl_snd,
    a_load, w_load, sc_load, res_load,
    a_send, a_recv, w_send, w_recv, sc_send, sc_recv,
    s1, r1, s2, r2, s3, r3, s4, r4, s5, r5,
):
    rows, depth = a_hbm.shape
    cols = w_hbm.shape[1]
    my_cols = hidden.shape[1]
    blocks = sc_hbm.shape[0]
    per_block = depth // blocks
    half, quarter = rows // 2, rows // 4
    inner, width, pieces, own, level, waves = plan(dp, groups, cols)
    segs = len(pieces)

    d = lax.axis_index("dp")
    t = lax.axis_index("tensor")
    z, i = d // inner, d % inner
    core, x = t % 2, t // 2
    core_peer = t + 1 - 2 * core
    x_peer = (t + 2) % 4

    def line(o):
        return {"dp": o * inner + i, "tensor": t}

    def row(other):
        return {"dp": d, "tensor": other}

    def pair(other):
        return {"dp": z * inner + other, "tensor": t}

    def step_block(j):
        if j == 0:
            return z
        if j == 1:
            return z + 1 - 2 * (z % 2)
        if j == 2:
            return z + 2 - 4 * (z // 2)
        return 3 - z

    def row_offset(who):
        return pl.multiple_of((who % 2) * half + (who // 2) * quarter, quarter)

    def seg_col(s):
        r, c, w = pieces[s]
        return pl.multiple_of(((i + r) % inner) * cols + c, w)

    def remote(src, dst, send, recv, to):
        return pltpu.make_async_remote_copy(
            src_ref=src, dst_ref=dst, send_sem=send, recv_sem=recv,
            device_id=to, device_id_type=MESH,
        )

    mine = row_offset(t)
    order = [t, x_peer, core_peer, (core_peer + 2) % 4]

    def load_a(q):
        return pltpu.make_async_copy(
            a_hbm.at[pl.ds(row_offset(order[q]), quarter), :],
            a_buf.at[z, pl.ds(q * quarter, quarter), :], a_load.at[q],
        )

    def load_w(s):
        _, c, w = pieces[s]
        return pltpu.make_async_copy(w_hbm.at[:, pl.ds(c, w)], w_buf.at[s, :, pl.ds(0, w)], w_load.at[s])

    sc_copy_in = pltpu.make_async_copy(sc_hbm, sc_buf.at[0], sc_load)
    res_copy = pltpu.make_async_copy(res_hbm.at[pl.ds(mine, quarter), :], res, res_load)
    for q in range(4):
        load_a(q).start()
    sc_copy_in.start()
    for s in range(own):
        load_w(s).start()
    res_copy.start()

    barrier = pltpu.get_barrier_semaphore()
    for r in range(1, inner):
        pl.semaphore_signal(barrier, inc=1, device_id=pair((i + r) % inner), device_id_type=MESH)
    for r in range(1, groups):
        pl.semaphore_signal(barrier, inc=1, device_id=line((z + r) % groups), device_id_type=MESH)
    for r in range(1, 4):
        pl.semaphore_signal(barrier, inc=1, device_id=row((t + r) % 4), device_id_type=MESH)
    pl.semaphore_wait(barrier, inner - 1 + groups - 1 + 3)

    size = rows // PARTS

    def a_copy(block, h, send, to):
        part = a_buf.at[block, pl.ds(h * size, size), :]
        return remote(part, part, a_send.at[send, h], a_recv.at[block, h], line(to))

    def sc_copy(r):
        return remote(sc_buf.at[0], sc_buf.at[r], sc_send.at[r - 1], sc_recv.at[r - 1], pair((i + inner - r) % inner))

    def w_copy(s):
        r, c, w = pieces[s]
        k, at = c // width, c % width
        return remote(
            w_buf.at[k, :, pl.ds(at, w)], w_buf.at[s, :, pl.ds(0, w)], w_send.at[s - own], w_recv.at[s - own],
            pair((i + inner - r) % inner),
        )

    for q in range(4):
        load_a(q).wait()
    for h in range(PARTS):
        @pl.when(z < groups - 1)
        def _():
            a_copy(z, h, z, z + 1).start()

        @pl.when(z > 0)
        def _():
            a_copy(z, h, groups, z - 1).start()

    sc_copy_in.wait()
    for r in range(1, inner):
        sc_copy(r).start()
    for s in range(own):
        load_w(s).wait()
    for s in range(own, segs):
        w_copy(s).start()

    def dequantize(s):
        r, c, w = pieces[s]
        for b in range(blocks):
            lines = pl.ds(b * per_block, per_block)
            raw = w_buf[s, lines, pl.ds(0, w)]
            scale = sc_buf[r, pl.ds(b, 1), pl.ds(c, w)]
            wd[s, lines, pl.ds(0, w)] = (raw.astype(jnp.float32) * scale).astype(jnp.bfloat16)

    def forward(k, h):
        @pl.when(z >= k)
        def _():
            b = z - k
            a_copy(b, h, b, z).wait_recv()

            @pl.when(z < groups - 1)
            def _():
                a_copy(b, h, b, z + 1).start()

        @pl.when(z + k <= groups - 1)
        def _():
            b = z + k
            a_copy(b, h, b, z).wait_recv()

            @pl.when(z > 0)
            def _():
                a_copy(b, h, b, z - 1).start()

    units = [unit for wave in waves for unit in wave]

    def piece(ref, u):
        return ref.at[u, :, pl.ds(0, pieces[units[u][1]][2])]

    def copy1(u):
        return remote(piece(snd1, u), piece(rcv1, u), s1.at[u], r1.at[u], row(core_peer))

    def copy2(u):
        return remote(piece(snd2, u), piece(rcv2, u), s2.at[u], r2.at[u], row(x_peer))

    def copy3(u):
        return remote(piece(snd3, u), piece(zin, u), s3.at[u], r3.at[u], line(step_block(units[u][0])))

    def place(who, s):
        return hidden.at[pl.ds(row_offset(who), quarter), pl.ds(seg_col(s), pieces[s][2])]

    def copy4(u):
        j, s = units[u]
        return remote(piece(hs, u), place(t, s), s4.at[u], r4.at[t * segs + s], row(step_block(j)))

    def keep4(u):
        return pltpu.make_async_copy(piece(hs, u), place(t, units[u][1]), s4.at[u])

    def stage1(u):
        j, s = units[u]
        w = pieces[s][2]
        part = jnp.dot(a_buf[step_block(j)], wd[s, :, pl.ds(0, w)], preferred_element_type=jnp.float32)
        snd1[u, :, pl.ds(0, w)] = part[half:].astype(jnp.bfloat16)
        copy1(u).start()
        keep1[u, :, pl.ds(0, w)] = part[:half]

    def stage2(u):
        w = pieces[units[u][1]][2]
        copy1(u).wait_recv()
        total = keep1[u, :, pl.ds(0, w)] + rcv1[u, :, pl.ds(0, w)].astype(jnp.float32)
        snd2[u, :, pl.ds(0, w)] = total[quarter:].astype(jnp.bfloat16)
        copy2(u).start()
        keep2[u, :, pl.ds(0, w)] = total[:quarter]

    def stage3(u):
        j, s = units[u]
        w = pieces[s][2]
        copy2(u).wait_recv()
        total = (keep2[u, :, pl.ds(0, w)] + rcv2[u, :, pl.ds(0, w)].astype(jnp.float32)).astype(jnp.bfloat16)
        if j == 0:
            zin[u, :, pl.ds(0, w)] = total
        else:
            snd3[u, :, pl.ds(0, w)] = total
            copy3(u).start()

    def stage4(u):
        j, s = units[u]
        w = pieces[s][2]
        if j > 0:
            copy3(u).wait_recv()
        source = step_block(j)
        at = pl.multiple_of(source * my_cols + seg_col(s), w)
        h = (zin[u, :, pl.ds(0, w)].astype(jnp.float32) + res[:, pl.ds(at, w)].astype(jnp.float32)).astype(jnp.bfloat16)
        hs[u, :, pl.ds(0, w)] = h

        @pl.when(source != t)
        def _():
            copy4(u).start()

        @pl.when(source == t)
        def _():
            keep4(u).start()

        wide = h.astype(jnp.float32)
        square = wide * wide
        total = acc[...]
        for k in range(w // LANES):
            total = total + square[:, k * LANES:(k + 1) * LANES]
        acc[...] = total

    acc[...] = jnp.zeros_like(acc)
    number = 0
    late = []

    def weights(at):
        for s in range(segs):
            if level[s] == at:
                r = pieces[s][0]
                if r > 0:
                    if pieces[s - 1][0] != r:
                        sc_copy(r).wait_recv()
                    w_copy(s).wait_recv()
                dequantize(s)

    for n, wave in enumerate(waves):
        now = list(range(number, number + len(wave)))
        number += len(wave)
        if 1 <= n < groups:
            forward(n, PARTS - 1)
        weights(n)
        for u in now:
            stage1(u)
        for u in now:
            stage2(u)
        if n == 0:
            res_copy.wait()
        if n + 1 < groups:
            for h in range(PARTS - 1):
                forward(n + 1, h)
        for u in now:
            stage3(u)
        for u in late:
            stage4(u)
        late = now
    for u in late:
        stage4(u)

    mean_square = jnp.sum(acc[...], axis=1, keepdims=True) / (my_cols * groups)
    scl_snd[...] = jnp.broadcast_to(lax.rsqrt(mean_square + 1e-05), scl_snd.shape)
    keep5 = pltpu.make_async_copy(scl_snd, scl.at[pl.ds(mine, quarter), :], s5.at[3])

    def copy5(r):
        return remote(
            scl_snd, scl.at[pl.ds(mine, quarter), :], s5.at[r - 1], r5.at[t], row((t + r) % 4)
        )

    for r in range(1, 4):
        copy5(r).start()
    keep5.start()

    @pl.when(z < groups - 1)
    def _():
        for h in range(PARTS):
            a_copy(z, h, z, z + 1).wait_send()

    @pl.when(z > 0)
    def _():
        for h in range(PARTS):
            a_copy(z, h, groups, z - 1).wait_send()

    for k in range(1, groups):
        @pl.when((z >= k) & (z < groups - 1))
        def _():
            for h in range(PARTS):
                a_copy(z - k, h, z - k, z + 1).wait_send()

        @pl.when((z + k <= groups - 1) & (z > 0))
        def _():
            for h in range(PARTS):
                a_copy(z + k, h, z + k, z - 1).wait_send()

    for r in range(1, inner):
        sc_copy(r).wait_send()
    for s in range(own, segs):
        w_copy(s).wait_send()
    for u, (j, s) in enumerate(units):
        copy1(u).wait_send()
        copy2(u).wait_send()
        if j > 0:
            copy3(u).wait_send()

    for r in range(1, 4):
        who = (t + r) % 4
        for s in range(segs):
            w = pieces[s][2]
            remote(hs.at[0, :, pl.ds(0, w)], place(who, s), s4.at[0], r4.at[who * segs + s], row(who)).wait_recv()
    for u, (j, s) in enumerate(units):
        @pl.when(step_block(j) != t)
        def _():
            copy4(u).wait_send()

        @pl.when(step_block(j) == t)
        def _():
            keep4(u).wait()
    for r in range(1, 4):
        who = (t + r) % 4
        remote(scl_snd, scl.at[pl.ds(row_offset(who), quarter), :], s5.at[0], r5.at[who], row(who)).wait_recv()
    for r in range(1, 4):
        copy5(r).wait_send()
    keep5.wait()


def finish(h_ref, scale_ref, gain_ref, hidden_ref, normed_ref):
    h = h_ref[...]
    hidden_ref[...] = h
    normed_ref[...] = (h.astype(jnp.float32) * gain_ref[...] * scale_ref[:, :1]).astype(jnp.bfloat16)


def solution(mesh):
    dp, groups = mesh.shape["dp"], mesh.shape["tensor"]

    def on_device(attn_out, w_blocks, w_scales, residual, gain):
        rows, depth = attn_out.shape
        cols = w_blocks.shape[1]
        my_cols = gain.shape[0]
        inner, width, pieces, own, level, waves = plan(dp, groups, cols)
        segs = len(pieces)
        n = segs * groups
        peers = segs - own
        half, quarter = rows // 2, rows // 4
        bf16, f32 = jnp.bfloat16, jnp.float32
        hbm = pl.BlockSpec(memory_space=pl.ANY)
        dma = pltpu.SemaphoreType.DMA
        out = jax.ShapeDtypeStruct((rows, my_cols), bf16)
        hidden, scale = pl.pallas_call(
            functools.partial(kernel, dp, groups),
            out_shape=(out, jax.ShapeDtypeStruct((rows, LANES), f32)),
            in_specs=[hbm] * 4,
            out_specs=(hbm, hbm),
            scratch_shapes=[
                pltpu.VMEM((groups, rows, depth), bf16),
                pltpu.VMEM((segs, depth, width), bf16),
                pltpu.VMEM((inner,) + w_scales.shape, f32),
                pltpu.VMEM((segs, depth, width), bf16),
                pltpu.VMEM((quarter, residual.shape[1]), bf16),
                pltpu.VMEM((n, half, width), f32),
                pltpu.VMEM((n, half, width), bf16),
                pltpu.VMEM((n, half, width), bf16),
                pltpu.VMEM((n, quarter, width), bf16),
                pltpu.VMEM((n, quarter, width), f32),
                pltpu.VMEM((n, quarter, width), bf16),
                pltpu.VMEM((n, quarter, width), bf16),
                pltpu.VMEM((n, quarter, width), bf16),
                pltpu.VMEM((n, quarter, width), bf16),
                pltpu.VMEM((quarter, LANES), f32),
                pltpu.VMEM((quarter, LANES), f32),
                dma((4,)), dma((own,)), dma, dma,
                dma((groups + 1, PARTS)), dma((groups, PARTS)), dma((peers,)), dma((peers,)),
                dma((inner - 1,)), dma((inner - 1,)),
                dma((n,)), dma((n,)), dma((n,)), dma((n,)), dma((n,)), dma((n,)),
                dma((n,)), dma((groups * segs,)), dma((4,)), dma((groups,)),
            ],
            compiler_params=pltpu.CompilerParams(
                collective_id=0, has_side_effects=True, vmem_limit_bytes=60 * 1024 * 1024,
            ),
        )(attn_out, w_blocks, w_scales, residual)
        tile = pl.BlockSpec((quarter, my_cols), lambda k: (k, 0))
        return pl.pallas_call(
            finish,
            grid=(4,),
            out_shape=(out, out),
            in_specs=[
                tile,
                pl.BlockSpec((quarter, LANES), lambda k: (k, 0)),
                pl.BlockSpec((1, my_cols), lambda k: (0, 0)),
            ],
            out_specs=(tile, tile),
        )(hidden, scale, gain[None, :])

    return jax.shard_map(
        on_device,
        mesh=mesh,
        in_specs=(
            P("dp", "tensor"),
            P("tensor", "dp"),
            P("tensor", "dp"),
            P("dp", None),
            P("tensor"),
        ),
        out_specs=(P("dp", "tensor"), P("dp", "tensor")),
        check_vma=False,
    )
```

```python
import functools

import jax
import jax.numpy as jnp
from jax import lax
from jax.experimental import pallas as pl
from jax.experimental.pallas import tpu as pltpu
from jax.sharding import PartitionSpec as P

MESH = pl.DeviceIdType.MESH
WIDTH = 256
LANES = 128
PARTS = 2
CHUNKS = 8


def plan(dp, groups, cols):
    inner = dp // groups
    width = min(WIDTH, cols)
    pieces = [(0, c, width) for c in range(0, cols, width)]
    own = len(pieces)
    for r in range(1, inner):
        for c in range(0, cols, width):
            if r == inner - 1 and c == cols - width and width > LANES:
                pieces += [(r, k, LANES) for k in range(c, cols, LANES)]
            else:
                pieces.append((r, c, width))
    units = [(j, s) for s in range(len(pieces)) for j in range(groups)]
    return inner, width, pieces, own, units


HOP, SWAP, START, TURN, DOT, CROSS = 11.3, 45.0, 4.5, 1.8, 0.42, 0.7


def steps(dp, groups, cols, middle):
    inner, width, pieces, own, units = plan(dp, groups, cols)
    far = [0, 1, 2, 1] if middle else [0, 1, 2, 3]
    total = sum(w for _, _, w in pieces[own:])
    got, weight = 0, []
    for r, _, w in pieces:
        got += w if r else 0
        weight.append(START + SWAP * got / total if r else 0.0)
    todo = []
    for k in range(1, groups):
        for h in range(PARTS):
            todo.append((START + HOP * (k - 1) + HOP * (h + 1) / PARTS, 0, "pass", k, h))
    token = [START + HOP * far[j] if far[j] else 0.0 for j in range(groups)]
    last = START + HOP * (groups - 1)
    ready = []
    for s in range(len(pieces)):
        if weight[s] >= last - 1:
            ready.append((max(last, weight[s]), -9, s, list(range(groups))[::-1]))
        else:
            ready += [(max(token[j], weight[s]), -far[j], s, [j]) for j in range(groups)]
    free = cross = 0.0
    seen = set()
    sent = START + HOP * 2 + 0.1
    for at, _, s, js in sorted(ready):
        size = pieces[s][2] / WIDTH
        free = max(free, at)
        if s not in seen:
            seen.add(s)
            todo.append((free, 1, "weights", s, 0))
        todo.append((free, 2, "dots" if len(js) > 1 else "dot", s, js))
        free += DOT * size * (1 if len(js) == 1 else 2)
        for j in js:
            u = s * groups + j
            todo.append((free + TURN, 3, "core", u, 0))
            cross = max(cross, free + TURN) + CROSS * size
            out = cross + TURN
            if j > 0 and out < sent:
                out = sent
            todo.append((out, 4, "x", u, 0))
    end = max(e[0] for e in todo)
    for s in range(len(pieces)):
        todo.append((end, 5, "add", s, 0))
    return [(name, u, h) for _, _, name, u, h in sorted(todo, key=lambda e: e[:2])]


def kernel(
    dp, groups,
    a_hbm, w_hbm, sc_hbm, res_hbm,
    hidden, scl,
    a_buf, w_buf, sc_buf, wd, res,
    keep1, snd1, rcv1, snd2, keep2, rcv2, snd3, zin, acc, sums,
    a_load, w_load, sc_load, res_load,
    a_send, a_recv, w_send, w_recv, sc_send, sc_recv,
    s1, r1, s2, r2, s3, r3, s5, r5,
):
    rows, depth = a_hbm.shape
    cols = w_hbm.shape[1]
    my_cols = hidden.shape[1]
    blocks = sc_hbm.shape[0]
    per_block = depth // blocks
    half, quarter = rows // 2, rows // 4
    inner, width, pieces, own, units = plan(dp, groups, cols)
    segs = len(pieces)

    d = lax.axis_index("dp")
    t = lax.axis_index("tensor")
    z, i = d // inner, d % inner
    core, x = t % 2, t // 2
    core_peer = t + 1 - 2 * core
    x_peer = (t + 2) % 4

    def line(o):
        return {"dp": o * inner + i, "tensor": t}

    def row(other):
        return {"dp": d, "tensor": other}

    def pair(other):
        return {"dp": z * inner + other, "tensor": t}

    def step_block(j):
        if j == 0:
            return z
        if j == 1:
            return z + 1 - 2 * (z % 2)
        if j == 2:
            return z + 2 - 4 * (z // 2)
        return 3 - z

    def row_offset(who):
        return pl.multiple_of((who % 2) * half + (who // 2) * quarter, quarter)

    def seg_col(s):
        r, c, w = pieces[s]
        return pl.multiple_of(((i + r) % inner) * cols + c, w)

    def remote(src, dst, send, recv, to):
        return pltpu.make_async_remote_copy(
            src_ref=src, dst_ref=dst, send_sem=send, recv_sem=recv,
            device_id=to, device_id_type=MESH,
        )

    mine = row_offset(t)
    order = [t, x_peer, core_peer, (core_peer + 2) % 4]

    def load_a(q):
        return pltpu.make_async_copy(
            a_hbm.at[pl.ds(row_offset(order[q]), quarter), :],
            a_buf.at[z, pl.ds(q * quarter, quarter), :], a_load.at[q],
        )

    def load_w(s):
        _, c, w = pieces[s]
        return pltpu.make_async_copy(w_hbm.at[:, pl.ds(c, w)], w_buf.at[s, :, pl.ds(0, w)], w_load.at[s])

    sc_copy_in = pltpu.make_async_copy(sc_hbm, sc_buf.at[0], sc_load)
    res_copy = pltpu.make_async_copy(
        res_hbm.at[:, pl.ds(pl.multiple_of(t * my_cols, my_cols), my_cols)], res, res_load
    )
    for q in range(4):
        load_a(q).start()
    sc_copy_in.start()
    for s in range(own):
        load_w(s).start()
    res_copy.start()

    barrier = pltpu.get_barrier_semaphore()
    for r in range(1, inner):
        pl.semaphore_signal(barrier, inc=1, device_id=pair((i + r) % inner), device_id_type=MESH)
    for r in range(1, groups):
        pl.semaphore_signal(barrier, inc=1, device_id=line((z + r) % groups), device_id_type=MESH)
    for r in range(1, 4):
        pl.semaphore_signal(barrier, inc=1, device_id=row((t + r) % 4), device_id_type=MESH)
    pl.semaphore_wait(barrier, inner - 1 + groups - 1 + 3)

    size = rows // PARTS

    def a_copy(block, h, send, to):
        part = a_buf.at[block, pl.ds(h * size, size), :]
        return remote(part, part, a_send.at[send, h], a_recv.at[block, h], line(to))

    def sc_copy(r):
        return remote(sc_buf.at[0], sc_buf.at[r], sc_send.at[r - 1], sc_recv.at[r - 1], pair((i + inner - r) % inner))

    def w_copy(s):
        r, c, w = pieces[s]
        k, at = c // width, c % width
        return remote(
            w_buf.at[k, :, pl.ds(at, w)], w_buf.at[s, :, pl.ds(0, w)], w_send.at[s - own], w_recv.at[s - own],
            pair((i + inner - r) % inner),
        )

    for q in range(4):
        load_a(q).wait()
    for h in range(PARTS):
        @pl.when(z < groups - 1)
        def _():
            a_copy(z, h, z, z + 1).start()

        @pl.when(z > 0)
        def _():
            a_copy(z, h, groups, z - 1).start()

    sc_copy_in.wait()
    for r in range(1, inner):
        sc_copy(r).start()
    landed = set()
    for s in range(own, segs):
        k = pieces[s][1] // width
        if k not in landed:
            landed.add(k)
            load_w(k).wait()
        w_copy(s).start()

    def dequantize(s):
        r, c, w = pieces[s]
        for b in range(blocks):
            lines = pl.ds(b * per_block, per_block)
            raw = w_buf[s, lines, pl.ds(0, w)]
            scale = sc_buf[r, pl.ds(b, 1), pl.ds(c, w)]
            wd[s, lines, pl.ds(0, w)] = (raw.astype(jnp.float32) * scale).astype(jnp.bfloat16)

    def forward(k, h):
        @pl.when(z >= k)
        def _():
            b = z - k
            a_copy(b, h, b, z).wait_recv()

            @pl.when(z < groups - 1)
            def _():
                a_copy(b, h, b, z + 1).start()

        @pl.when(z + k <= groups - 1)
        def _():
            b = z + k
            a_copy(b, h, b, z).wait_recv()

            @pl.when(z > 0)
            def _():
                a_copy(b, h, b, z - 1).start()

    def piece(ref, u):
        return ref.at[u, :, pl.ds(0, pieces[units[u][1]][2])]

    def copy1(u):
        return remote(piece(snd1, u), piece(rcv1, u), s1.at[u], r1.at[u], row(core_peer))

    def copy2(u):
        return remote(piece(snd2, u), piece(rcv2, u), s2.at[u], r2.at[u], row(x_peer))

    def spot(who, s):
        return zin.at[s, pl.ds(row_offset(who), quarter), pl.ds(0, pieces[s][2])]

    def copy3(u):
        j, s = units[u]
        to = {"dp": step_block(j) * inner + i, "tensor": z}
        return remote(piece(snd3, u), spot(t, s), s3.at[u], r3.at[s, t], to)

    def stage1(u):
        j, s = units[u]
        w = pieces[s][2]
        part = jnp.dot(a_buf[step_block(j)], wd[s, :, pl.ds(0, w)], preferred_element_type=jnp.float32)
        snd1[u, :, pl.ds(0, w)] = part[half:].astype(jnp.bfloat16)
        copy1(u).start()
        keep1[u, :, pl.ds(0, w)] = part[:half]

    def stage1_all(s, js):
        w = pieces[s][2]
        tokens = a_buf[...].reshape(groups * rows, depth)
        part = jnp.dot(tokens, wd[s, :, pl.ds(0, w)], preferred_element_type=jnp.float32)
        for b in range(groups):
            u = s * groups + step_block(b)
            snd1[u, :, pl.ds(0, w)] = part[b * rows + half:(b + 1) * rows].astype(jnp.bfloat16)
            keep1[u, :, pl.ds(0, w)] = part[b * rows:b * rows + half]
        for j in js:
            copy1(s * groups + j).start()

    def stage2(u):
        w = pieces[units[u][1]][2]
        copy1(u).wait_recv()
        total = keep1[u, :, pl.ds(0, w)] + rcv1[u, :, pl.ds(0, w)].astype(jnp.float32)
        snd2[u, :, pl.ds(0, w)] = total[quarter:].astype(jnp.bfloat16)
        copy2(u).start()
        keep2[u, :, pl.ds(0, w)] = total[:quarter]

    def stage3(u):
        j, s = units[u]
        w = pieces[s][2]
        copy2(u).wait_recv()
        total = (keep2[u, :, pl.ds(0, w)] + rcv2[u, :, pl.ds(0, w)].astype(jnp.float32)).astype(jnp.bfloat16)
        if j > 0:
            snd3[u, :, pl.ds(0, w)] = total
            copy3(u).start()
        else:
            @pl.when(z == t)
            def _():
                zin[s, pl.ds(mine, quarter), pl.ds(0, w)] = total

            @pl.when(z != t)
            def _():
                snd3[u, :, pl.ds(0, w)] = total
                copy3(u).start()

    def stage4(s):
        w = pieces[s][2]
        for who in range(4):
            @pl.when((z != t) | (t != who))
            def _():
                remote(piece(snd3, s * groups), spot(who, s), s3.at[0], r3.at[s, who], row(who)).wait_recv()
        at = pl.ds(seg_col(s), w)
        h = (zin[s, :, pl.ds(0, w)].astype(jnp.float32) + res[:, at].astype(jnp.float32)).astype(jnp.bfloat16)
        hidden[:, at] = h
        wide = h.astype(jnp.float32)
        square = wide * wide
        total = acc[...]
        for k in range(w // LANES):
            total = total + square[:, k * LANES:(k + 1) * LANES]
        acc[...] = total

    acc[...] = jnp.zeros_like(acc)

    def weights(s):
        r = pieces[s][0]
        if r > 0:
            if pieces[s - 1][0] != r:
                sc_copy(r).wait_recv()
            w_copy(s).wait_recv()
        dequantize(s)

    res_copy.wait()

    def run(middle):
        for name, u, h in steps(dp, groups, cols, middle):
            if name == "pass":
                forward(u, h)
            elif name == "weights":
                weights(u)
            elif name == "dot":
                stage1(u * groups + h[0])
            elif name == "dots":
                stage1_all(u, h)
            elif name == "core":
                stage2(u)
            elif name == "x":
                stage3(u)
            else:
                stage4(u)

    outer = (z == 0) | (z == groups - 1)
    pl.when(outer)(lambda: run(False))
    pl.when(jnp.logical_not(outer))(lambda: run(True))

    exact = lax.Precision.HIGHEST
    sums[t] = lax.dot_general(
        jnp.ones((8, LANES), jnp.float32), acc[...], (((1,), (1,)), ((), ())),
        precision=exact, preferred_element_type=jnp.float32,
    )

    def copy5(r):
        return remote(sums.at[t], sums.at[t], s5.at[r - 1], r5.at[t], row((t + r) % 4))

    for r in range(1, 4):
        copy5(r).start()

    @pl.when(z < groups - 1)
    def _():
        for h in range(PARTS):
            a_copy(z, h, z, z + 1).wait_send()

    @pl.when(z > 0)
    def _():
        for h in range(PARTS):
            a_copy(z, h, groups, z - 1).wait_send()

    for k in range(1, groups):
        @pl.when((z >= k) & (z < groups - 1))
        def _():
            for h in range(PARTS):
                a_copy(z - k, h, z - k, z + 1).wait_send()

        @pl.when((z + k <= groups - 1) & (z > 0))
        def _():
            for h in range(PARTS):
                a_copy(z + k, h, z + k, z - 1).wait_send()

    for r in range(1, inner):
        sc_copy(r).wait_send()
    for s in range(own, segs):
        w_copy(s).wait_send()
    for u, (j, s) in enumerate(units):
        copy1(u).wait_send()
        copy2(u).wait_send()

        @pl.when((z != t) | (j > 0))
        def _():
            copy3(u).wait_send()

    for r in range(1, 4):
        who = (t + r) % 4
        remote(sums.at[t], sums.at[who], s5.at[0], r5.at[who], row(who)).wait_recv()
    for r in range(1, 4):
        copy5(r).wait_send()
    mean_square = (sums[0] + sums[1] + sums[2] + sums[3]) / (my_cols * groups)
    first = (lax.broadcasted_iota(jnp.int32, (8, LANES), 0) == 0).astype(jnp.float32)
    scl[...] = lax.dot_general(
        lax.rsqrt(mean_square + 1e-05), first, (((0,), (0,)), ((), ())),
        precision=exact, preferred_element_type=jnp.float32,
    )


def finish(chunks, h_ref, scale_ref, gain_ref, hidden_hbm, normed_hbm, normed, sems):
    size = h_ref.shape[0] // chunks
    copies = [pltpu.make_async_copy(h_ref, hidden_hbm, sems.at[chunks])]
    copies[0].start()
    for k in range(chunks):
        at = pl.ds(k * size, size)
        wide = h_ref[at, :].astype(jnp.float32)
        normed[at, :] = (wide * gain_ref[...] * scale_ref[at, :1]).astype(jnp.bfloat16)
        copies.append(pltpu.make_async_copy(normed.at[at, :], normed_hbm.at[at, :], sems.at[k]))
        copies[-1].start()
    for copy in copies:
        copy.wait()


def solution(mesh):
    dp, groups = mesh.shape["dp"], mesh.shape["tensor"]

    def on_device(attn_out, w_blocks, w_scales, residual, gain):
        rows, depth = attn_out.shape
        cols = w_blocks.shape[1]
        my_cols = gain.shape[0]
        inner, width, pieces, own, units = plan(dp, groups, cols)
        segs = len(pieces)
        n = len(units)
        peers = segs - own
        half, quarter = rows // 2, rows // 4
        bf16, f32 = jnp.bfloat16, jnp.float32
        hbm = pl.BlockSpec(memory_space=pltpu.MemorySpace.HBM)
        vmem = pl.BlockSpec(memory_space=pltpu.VMEM)
        dma = pltpu.SemaphoreType.DMA
        out = jax.ShapeDtypeStruct((rows, my_cols), bf16)
        hidden, scale = pl.pallas_call(
            functools.partial(kernel, dp, groups),
            out_shape=(out, jax.ShapeDtypeStruct((rows, LANES), f32)),
            in_specs=[hbm] * 4,
            out_specs=(vmem, vmem),
            scratch_shapes=[
                pltpu.VMEM((groups, rows, depth), bf16),
                pltpu.VMEM((segs, depth, width), bf16),
                pltpu.VMEM((inner,) + w_scales.shape, f32),
                pltpu.VMEM((segs, depth, width), bf16),
                pltpu.VMEM((rows, my_cols), bf16),
                pltpu.VMEM((n, half, width), f32),
                pltpu.VMEM((n, half, width), bf16),
                pltpu.VMEM((n, half, width), bf16),
                pltpu.VMEM((n, quarter, width), bf16),
                pltpu.VMEM((n, quarter, width), f32),
                pltpu.VMEM((n, quarter, width), bf16),
                pltpu.VMEM((n, quarter, width), bf16),
                pltpu.VMEM((segs, rows, width), bf16),
                pltpu.VMEM((rows, LANES), f32),
                pltpu.VMEM((groups, 8, rows), f32),
                dma((4,)), dma((own,)), dma, dma,
                dma((groups + 1, PARTS)), dma((groups, PARTS)), dma((peers,)), dma((peers,)),
                dma((inner - 1,)), dma((inner - 1,)),
                dma((n,)), dma((n,)), dma((n,)), dma((n,)), dma((n,)), dma((segs, groups)),
                dma((3,)), dma((groups,)),
            ],
            compiler_params=pltpu.CompilerParams(
                collective_id=0, has_side_effects=True, vmem_limit_bytes=48 * 1024 * 1024,
            ),
        )(*[pltpu.with_memory_space_constraint(v, pltpu.MemorySpace.HBM) for v in (attn_out, w_blocks, w_scales, residual)])
        return pl.pallas_call(
            functools.partial(finish, CHUNKS),
            out_shape=(out, out),
            in_specs=[vmem] * 3,
            out_specs=(hbm, hbm),
            scratch_shapes=[pltpu.VMEM((rows, my_cols), bf16), dma((CHUNKS + 1,))],
            compiler_params=pltpu.CompilerParams(vmem_limit_bytes=16 * 1024 * 1024),
        )(hidden, scale, gain[None, :])

    return jax.shard_map(
        on_device,
        mesh=mesh,
        in_specs=(
            P("dp", "tensor"),
            P("tensor", "dp"),
            P("tensor", "dp"),
            P("dp", None),
            P("tensor"),
        ),
        out_specs=(P("dp", "tensor"), P("dp", "tensor")),
        check_vma=False,
    )
```

```python
import functools

import jax
import jax.numpy as jnp
from jax import lax
from jax.experimental import pallas as pl
from jax.experimental.pallas import tpu as pltpu
from jax.sharding import PartitionSpec as P

MESH = pl.DeviceIdType.MESH
WIDTH = 256
LANES = 128
PARTS = 2
CHUNKS = 8
WHOLE = 3


def plan(dp, groups, cols):
    inner = dp // groups
    width = min(WIDTH, cols)
    pieces = [(0, c, width) for c in range(0, cols, width)]
    own = len(pieces)
    for r in range(1, inner):
        for c in range(0, cols, width):
            if r == inner - 1 and c == cols - width and width > LANES:
                pieces += [(r, k, LANES) for k in range(c, cols, LANES)]
            else:
                pieces.append((r, c, width))
    units = [(j, s) for s in range(len(pieces)) for j in range(groups)]
    return inner, width, pieces, own, units


def direct(groups, own, u, middle):
    return not middle and u % groups == groups - 1 and u // groups < -(-own * WHOLE // 4)


HOP, SWAP, START, TURN, DOT, CROSS, SLACK = 11.3, 45.0, 4.5, 1.8, 0.42, 0.8, 1.0


def steps(dp, groups, cols, middle):
    inner, width, pieces, own, units = plan(dp, groups, cols)
    far = [0, 1, 2, 1] if middle else [0, 1, 2, 3]
    total = sum(w for _, _, w in pieces[own:])
    got, weight = 0, []
    for r, _, w in pieces:
        got += w if r else 0
        weight.append(START + SWAP * got / total if r else 0.0)
    todo = []
    for k in range(1, groups):
        for h in range(PARTS):
            todo.append((START + HOP * (k - 1) + HOP * (h + 1) / PARTS, 0, "pass", k, h))
    token = [START + HOP * far[j] if far[j] else 0.0 for j in range(groups)]
    last = START + HOP * (groups - 1)
    ready = []
    for s in range(len(pieces)):
        if weight[s] >= last - 1:
            ready.append((max(last, weight[s]), -9, s, list(range(groups))[::-1]))
        else:
            ready += [(max(token[j], weight[s]), -far[j], s, [j]) for j in range(groups)]
    free = cross = 0.0
    seen = set()
    sent = START + HOP * 2 + 0.1
    for at, _, s, js in sorted(ready):
        size = pieces[s][2] / WIDTH
        free = max(free, at)
        if s not in seen:
            seen.add(s)
            todo.append((free, 1, "weights", s, 0))
        todo.append((free, 2, "dots" if len(js) > 1 else "dot", s, js))
        free += DOT * size * (1 if len(js) == 1 else 2)
        for j in js:
            u = s * groups + j
            todo.append((free + TURN, 3, "core", u, 0))
            wide = 2 if direct(groups, own, u, middle) else 1
            cross = max(cross, free + TURN) + CROSS * size * wide
            out = cross + TURN + SLACK
            if j > 0 and out < sent:
                out = sent
            todo.append((out, 4, "x", u, 0))
    end = max(e[0] for e in todo)
    for s in range(len(pieces)):
        todo.append((end, 5, "add", s, 0))
    return [(name, u, h) for _, _, name, u, h in sorted(todo, key=lambda e: e[:2])]


def kernel(
    dp, groups,
    a_hbm, w_hbm, sc_hbm, res_hbm,
    hidden, scl,
    a_buf, w_buf, sc_buf, wd, res,
    keep1, snd1, rcv1, snd2, keep2, rcv2, snd3, sndh, rcvh, zin, acc, sums,
    a_load, w_load, sc_load, res_load,
    a_send, a_recv, w_send, w_recv, sc_send, sc_recv,
    s1, r1, s2, r2, s3, s3h, r3, s5, r5,
):
    rows, depth = a_hbm.shape
    cols = w_hbm.shape[1]
    my_cols = hidden.shape[1]
    blocks = sc_hbm.shape[0]
    per_block = depth // blocks
    half, quarter = rows // 2, rows // 4
    inner, width, pieces, own, units = plan(dp, groups, cols)
    segs = len(pieces)

    d = lax.axis_index("dp")
    t = lax.axis_index("tensor")
    z, i = d // inner, d % inner
    core, x = t % 2, t // 2
    core_peer = t + 1 - 2 * core
    x_peer = (t + 2) % 4

    def line(o):
        return {"dp": o * inner + i, "tensor": t}

    def row(other):
        return {"dp": d, "tensor": other}

    def pair(other):
        return {"dp": z * inner + other, "tensor": t}

    def step_block(j):
        if j == 0:
            return z
        if j == 1:
            return z + 1 - 2 * (z % 2)
        if j == 2:
            return z + 2 - 4 * (z // 2)
        return 3 - z

    def row_offset(who):
        return pl.multiple_of((who % 2) * half + (who // 2) * quarter, quarter)

    def seg_col(s):
        r, c, w = pieces[s]
        return pl.multiple_of(((i + r) % inner) * cols + c, w)

    def remote(src, dst, send, recv, to):
        return pltpu.make_async_remote_copy(
            src_ref=src, dst_ref=dst, send_sem=send, recv_sem=recv,
            device_id=to, device_id_type=MESH,
        )

    mine = row_offset(t)
    order = [t, x_peer, core_peer, (core_peer + 2) % 4]

    def load_a(q):
        return pltpu.make_async_copy(
            a_hbm.at[pl.ds(row_offset(order[q]), quarter), :],
            a_buf.at[z, pl.ds(q * quarter, quarter), :], a_load.at[q],
        )

    def load_w(s):
        _, c, w = pieces[s]
        return pltpu.make_async_copy(w_hbm.at[:, pl.ds(c, w)], w_buf.at[s, :, pl.ds(0, w)], w_load.at[s])

    sc_copy_in = pltpu.make_async_copy(sc_hbm, sc_buf.at[0], sc_load)
    res_copy = pltpu.make_async_copy(
        res_hbm.at[:, pl.ds(pl.multiple_of(t * my_cols, my_cols), my_cols)], res, res_load
    )
    for q in range(4):
        load_a(q).start()
    sc_copy_in.start()
    for s in range(own):
        load_w(s).start()
    res_copy.start()

    barrier = pltpu.get_barrier_semaphore()
    for r in range(1, inner):
        pl.semaphore_signal(barrier, inc=1, device_id=pair((i + r) % inner), device_id_type=MESH)
    for r in range(1, groups):
        pl.semaphore_signal(barrier, inc=1, device_id=line((z + r) % groups), device_id_type=MESH)
    for r in range(1, 4):
        pl.semaphore_signal(barrier, inc=1, device_id=row((t + r) % 4), device_id_type=MESH)
    pl.semaphore_wait(barrier, inner - 1 + groups - 1 + 3)

    size = rows // PARTS

    def a_copy(block, h, send, to):
        part = a_buf.at[block, pl.ds(h * size, size), :]
        return remote(part, part, a_send.at[send, h], a_recv.at[block, h], line(to))

    def sc_copy(r):
        return remote(sc_buf.at[0], sc_buf.at[r], sc_send.at[r - 1], sc_recv.at[r - 1], pair((i + inner - r) % inner))

    def w_copy(s):
        r, c, w = pieces[s]
        k, at = c // width, c % width
        return remote(
            w_buf.at[k, :, pl.ds(at, w)], w_buf.at[s, :, pl.ds(0, w)], w_send.at[s - own], w_recv.at[s - own],
            pair((i + inner - r) % inner),
        )

    for q in range(4):
        load_a(q).wait()
    for h in range(PARTS):
        @pl.when(z < groups - 1)
        def _():
            a_copy(z, h, z, z + 1).start()

        @pl.when(z > 0)
        def _():
            a_copy(z, h, groups, z - 1).start()

    sc_copy_in.wait()
    for r in range(1, inner):
        sc_copy(r).start()
    landed = set()
    for s in range(own, segs):
        k = pieces[s][1] // width
        if k not in landed:
            landed.add(k)
            load_w(k).wait()
        w_copy(s).start()

    def dequantize(s):
        r, c, w = pieces[s]
        for b in range(blocks):
            lines = pl.ds(b * per_block, per_block)
            raw = w_buf[s, lines, pl.ds(0, w)]
            scale = sc_buf[r, pl.ds(b, 1), pl.ds(c, w)]
            wd[s, lines, pl.ds(0, w)] = (raw.astype(jnp.float32) * scale).astype(jnp.bfloat16)

    def forward(k, h):
        @pl.when(z >= k)
        def _():
            b = z - k
            a_copy(b, h, b, z).wait_recv()

            @pl.when(z < groups - 1)
            def _():
                a_copy(b, h, b, z + 1).start()

        @pl.when(z + k <= groups - 1)
        def _():
            b = z + k
            a_copy(b, h, b, z).wait_recv()

            @pl.when(z > 0)
            def _():
                a_copy(b, h, b, z - 1).start()

    def piece(ref, u):
        return ref.at[u, :, pl.ds(0, pieces[units[u][1]][2])]

    def copy1(u):
        return remote(piece(snd1, u), piece(rcv1, u), s1.at[u], r1.at[u], row(core_peer))

    def slot(ref, u):
        return ref.at[units[u][1], :, pl.ds(0, pieces[units[u][1]][2])]

    def copy2h(u):
        return remote(slot(sndh, u), slot(rcvh, u), s2.at[u], r2.at[u], row(x_peer))

    def copy3h(u, q):
        j, s = units[u]
        to = {"dp": step_block(j) * inner + i, "tensor": z}
        part = sndh.at[s, pl.ds(q * quarter, quarter), pl.ds(0, pieces[s][2])]
        return remote(part, spot([t, x_peer][q], s), [s3, s3h][q].at[u], r3.at[s, [t, x_peer][q]], to)

    def copy2(u):
        return remote(piece(snd2, u), piece(rcv2, u), s2.at[u], r2.at[u], row(x_peer))

    def spot(who, s):
        return zin.at[s, pl.ds(row_offset(who), quarter), pl.ds(0, pieces[s][2])]

    def copy3(u):
        j, s = units[u]
        to = {"dp": step_block(j) * inner + i, "tensor": z}
        return remote(piece(snd3, u), spot(t, s), s3.at[u], r3.at[s, t], to)

    def stage1(u):
        j, s = units[u]
        w = pieces[s][2]
        part = jnp.dot(a_buf[step_block(j)], wd[s, :, pl.ds(0, w)], preferred_element_type=jnp.float32)
        snd1[u, :, pl.ds(0, w)] = part[half:].astype(jnp.bfloat16)
        copy1(u).start()
        keep1[u, :, pl.ds(0, w)] = part[:half]

    def stage1_all(s, js):
        w = pieces[s][2]
        tokens = a_buf[...].reshape(groups * rows, depth)
        part = jnp.dot(tokens, wd[s, :, pl.ds(0, w)], preferred_element_type=jnp.float32)
        for b in range(groups):
            u = s * groups + step_block(b)
            snd1[u, :, pl.ds(0, w)] = part[b * rows + half:(b + 1) * rows].astype(jnp.bfloat16)
            keep1[u, :, pl.ds(0, w)] = part[b * rows:b * rows + half]
        for j in js:
            copy1(s * groups + j).start()

    def stage2(u, middle):
        w = pieces[units[u][1]][2]
        copy1(u).wait_recv()
        total = keep1[u, :, pl.ds(0, w)] + rcv1[u, :, pl.ds(0, w)].astype(jnp.float32)
        if direct(groups, own, u, middle):
            at = units[u][1]

            @pl.when(x == z // 2)
            def _():
                keep1[u, :, pl.ds(0, w)] = total

            @pl.when(x != z // 2)
            def _():
                sndh[at, pl.ds(0, quarter), pl.ds(0, w)] = total[quarter:].astype(jnp.bfloat16)
                sndh[at, pl.ds(quarter, quarter), pl.ds(0, w)] = total[:quarter].astype(jnp.bfloat16)
                copy2h(u).start()

            return
        snd2[u, :, pl.ds(0, w)] = total[quarter:].astype(jnp.bfloat16)
        copy2(u).start()
        keep2[u, :, pl.ds(0, w)] = total[:quarter]

    def stage3(u, middle):
        j, s = units[u]
        w = pieces[s][2]
        if direct(groups, own, u, middle):
            @pl.when(x == z // 2)
            def _():
                copy2h(u).wait_recv()
                both = keep1[u, :, pl.ds(0, w)] + rcvh[s, :, pl.ds(0, w)].astype(jnp.float32)
                sndh[s, :, pl.ds(0, w)] = both.astype(jnp.bfloat16)
                for q in range(2):
                    copy3h(u, q).start()

            return
        copy2(u).wait_recv()
        total = (keep2[u, :, pl.ds(0, w)] + rcv2[u, :, pl.ds(0, w)].astype(jnp.float32)).astype(jnp.bfloat16)
        if j > 0:
            snd3[u, :, pl.ds(0, w)] = total
            copy3(u).start()
        else:
            @pl.when(z == t)
            def _():
                zin[s, pl.ds(mine, quarter), pl.ds(0, w)] = total

            @pl.when(z != t)
            def _():
                snd3[u, :, pl.ds(0, w)] = total
                copy3(u).start()

    def stage4(s):
        w = pieces[s][2]
        for who in range(4):
            @pl.when((z != t) | (t != who))
            def _():
                remote(piece(snd3, s * groups), spot(who, s), s3.at[0], r3.at[s, who], row(who)).wait_recv()
        at = pl.ds(seg_col(s), w)
        h = (zin[s, :, pl.ds(0, w)].astype(jnp.float32) + res[:, at].astype(jnp.float32)).astype(jnp.bfloat16)
        hidden[:, at] = h
        wide = h.astype(jnp.float32)
        square = wide * wide
        total = acc[...]
        for k in range(w // LANES):
            total = total + square[:, k * LANES:(k + 1) * LANES]
        acc[...] = total

    acc[...] = jnp.zeros_like(acc)

    def weights(s):
        r = pieces[s][0]
        if r > 0:
            if pieces[s - 1][0] != r:
                sc_copy(r).wait_recv()
            w_copy(s).wait_recv()
        dequantize(s)

    res_copy.wait()

    def run(middle):
        for name, u, h in steps(dp, groups, cols, middle):
            if name == "pass":
                forward(u, h)
            elif name == "weights":
                weights(u)
            elif name == "dot":
                stage1(u * groups + h[0])
            elif name == "dots":
                stage1_all(u, h)
            elif name == "core":
                stage2(u, middle)
            elif name == "x":
                stage3(u, middle)
            else:
                stage4(u)

    outer = (z == 0) | (z == groups - 1)
    pl.when(outer)(lambda: run(False))
    pl.when(jnp.logical_not(outer))(lambda: run(True))

    exact = lax.Precision.HIGHEST
    sums[t] = lax.dot_general(
        jnp.ones((8, LANES), jnp.float32), acc[...], (((1,), (1,)), ((), ())),
        precision=exact, preferred_element_type=jnp.float32,
    )

    def copy5(r):
        return remote(sums.at[t], sums.at[t], s5.at[r - 1], r5.at[t], row((t + r) % 4))

    for r in range(1, 4):
        copy5(r).start()

    @pl.when(z < groups - 1)
    def _():
        for h in range(PARTS):
            a_copy(z, h, z, z + 1).wait_send()

    @pl.when(z > 0)
    def _():
        for h in range(PARTS):
            a_copy(z, h, groups, z - 1).wait_send()

    for k in range(1, groups):
        @pl.when((z >= k) & (z < groups - 1))
        def _():
            for h in range(PARTS):
                a_copy(z - k, h, z - k, z + 1).wait_send()

        @pl.when((z + k <= groups - 1) & (z > 0))
        def _():
            for h in range(PARTS):
                a_copy(z + k, h, z + k, z - 1).wait_send()

    for r in range(1, inner):
        sc_copy(r).wait_send()
    for s in range(own, segs):
        w_copy(s).wait_send()
    for u, (j, s) in enumerate(units):
        copy1(u).wait_send()

        def plain(u=u, j=j):
            copy2(u).wait_send()

            @pl.when((z != t) | (j > 0))
            def _():
                copy3(u).wait_send()

        if direct(groups, own, u, False):
            @pl.when(outer & (x == z // 2))
            def _():
                for q in range(2):
                    copy3h(u, q).wait_send()

            @pl.when(outer & (x != z // 2))
            def _():
                copy2h(u).wait_send()

            pl.when(jnp.logical_not(outer))(plain)
        else:
            plain()

    for r in range(1, 4):
        who = (t + r) % 4
        remote(sums.at[t], sums.at[who], s5.at[0], r5.at[who], row(who)).wait_recv()
    for r in range(1, 4):
        copy5(r).wait_send()
    mean_square = (sums[0] + sums[1] + sums[2] + sums[3]) / (my_cols * groups)
    first = (lax.broadcasted_iota(jnp.int32, (8, LANES), 0) == 0).astype(jnp.float32)
    scl[...] = lax.dot_general(
        lax.rsqrt(mean_square + 1e-05), first, (((0,), (0,)), ((), ())),
        precision=exact, preferred_element_type=jnp.float32,
    )


def finish(chunks, h_ref, scale_ref, gain_ref, hidden_hbm, normed_hbm, normed, sems):
    size = h_ref.shape[0] // chunks
    copies = [pltpu.make_async_copy(h_ref, hidden_hbm, sems.at[chunks])]
    copies[0].start()
    for k in range(chunks):
        at = pl.ds(k * size, size)
        wide = h_ref[at, :].astype(jnp.float32)
        normed[at, :] = (wide * gain_ref[...] * scale_ref[at, :1]).astype(jnp.bfloat16)
        copies.append(pltpu.make_async_copy(normed.at[at, :], normed_hbm.at[at, :], sems.at[k]))
        copies[-1].start()
    for copy in copies:
        copy.wait()


def solution(mesh):
    dp, groups = mesh.shape["dp"], mesh.shape["tensor"]

    def on_device(attn_out, w_blocks, w_scales, residual, gain):
        rows, depth = attn_out.shape
        cols = w_blocks.shape[1]
        my_cols = gain.shape[0]
        inner, width, pieces, own, units = plan(dp, groups, cols)
        segs = len(pieces)
        n = len(units)
        peers = segs - own
        half, quarter = rows // 2, rows // 4
        bf16, f32 = jnp.bfloat16, jnp.float32
        hbm = pl.BlockSpec(memory_space=pltpu.MemorySpace.HBM)
        vmem = pl.BlockSpec(memory_space=pltpu.VMEM)
        dma = pltpu.SemaphoreType.DMA
        out = jax.ShapeDtypeStruct((rows, my_cols), bf16)
        hidden, scale = pl.pallas_call(
            functools.partial(kernel, dp, groups),
            out_shape=(out, jax.ShapeDtypeStruct((rows, LANES), f32)),
            in_specs=[hbm] * 4,
            out_specs=(vmem, vmem),
            scratch_shapes=[
                pltpu.VMEM((groups, rows, depth), bf16),
                pltpu.VMEM((segs, depth, width), bf16),
                pltpu.VMEM((inner,) + w_scales.shape, f32),
                pltpu.VMEM((segs, depth, width), bf16),
                pltpu.VMEM((rows, my_cols), bf16),
                pltpu.VMEM((n, half, width), f32),
                pltpu.VMEM((n, half, width), bf16),
                pltpu.VMEM((n, half, width), bf16),
                pltpu.VMEM((n, quarter, width), bf16),
                pltpu.VMEM((n, quarter, width), f32),
                pltpu.VMEM((n, quarter, width), bf16),
                pltpu.VMEM((n, quarter, width), bf16),
                pltpu.VMEM((-(-own * WHOLE // 4), half, width), bf16),
                pltpu.VMEM((-(-own * WHOLE // 4), half, width), bf16),
                pltpu.VMEM((segs, rows, width), bf16),
                pltpu.VMEM((rows, LANES), f32),
                pltpu.VMEM((groups, 8, rows), f32),
                dma((4,)), dma((own,)), dma, dma,
                dma((groups + 1, PARTS)), dma((groups, PARTS)), dma((peers,)), dma((peers,)),
                dma((inner - 1,)), dma((inner - 1,)),
                dma((n,)), dma((n,)), dma((n,)), dma((n,)), dma((n,)), dma((n,)), dma((segs, groups)),
                dma((3,)), dma((groups,)),
            ],
            compiler_params=pltpu.CompilerParams(
                collective_id=0, has_side_effects=True, vmem_limit_bytes=48 * 1024 * 1024,
            ),
        )(*[pltpu.with_memory_space_constraint(v, pltpu.MemorySpace.HBM) for v in (attn_out, w_blocks, w_scales, residual)])
        return pl.pallas_call(
            functools.partial(finish, CHUNKS),
            out_shape=(out, out),
            in_specs=[vmem] * 3,
            out_specs=(hbm, hbm),
            scratch_shapes=[pltpu.VMEM((rows, my_cols), bf16), dma((CHUNKS + 1,))],
            compiler_params=pltpu.CompilerParams(vmem_limit_bytes=16 * 1024 * 1024),
        )(hidden, scale, gain[None, :])

    return jax.shard_map(
        on_device,
        mesh=mesh,
        in_specs=(
            P("dp", "tensor"),
            P("tensor", "dp"),
            P("tensor", "dp"),
            P("dp", None),
            P("tensor"),
        ),
        out_specs=(P("dp", "tensor"), P("dp", "tensor")),
        check_vma=False,
    )
```
